32 devices in a mesh: job: 4 (over y, x), dp: 2 (over core), tp: 4 (over z).
Axes of the slice: x: 2, y: 2, z: 4, core: 2. Of those that a mesh axis runs over, the one named last changes fastest.
Arguments:
- partial_up: float32 [8, 768, 3072], P(('job', 'dp'), None, 'tp'), parts along dimension 0, may hold values from -0.875 to 0.875
- partial_down: float32 [8, 3072, 768], P(('job', 'dp'), 'tp'), parts along dimension 0, may hold values from -0.875 to 0.875
- partial_norm: float32 [8, 768], P(('job', 'dp')), parts along dimension 0, may hold values from -8 to 8
- partial_bias: float32 [8, 768], P(('job', 'dp')), parts along dimension 0, may hold values from -8 to 8
- master_up: float32 [3072, 3072], P(('job', 'dp'), 'tp'), parts along dimension 0, may hold values from -0.3125 to 0.3125
- master_down: float32 [12288, 768], P(('job', 'tp'), 'dp'), parts along dimension 0, may hold values from -0.15625 to 0.15625
- master_norm: float32 [3072], P(('job', 'dp')), parts along dimension 0, may hold values from 0.25 to 1.75
- master_bias: float32 [3072], P(('job', 'dp')), parts along dimension 0, may hold values from -3 to 3
- memory_up: float32 [3072, 3072], P(('job', 'dp'), 'tp'), parts along dimension 0, may hold values from -0.21875 to 0.21875
- memory_down: float32 [12288, 768], P(('job', 'tp'), 'dp'), parts along dimension 0, may hold values from -0.109375 to 0.109375
- memory_norm: float32 [3072], P(('job', 'dp')), parts along dimension 0, may hold values from -1.75 to 1.75
- memory_bias: float32 [3072], P(('job', 'dp')), parts along dimension 0, may hold values from -1.75 to 1.75
Outputs:
- compute_up: bfloat16 [3072, 3072], P('job', 'tp'), parts along dimension 0
- compute_down: bfloat16 [12288, 768], P(('job', 'tp')), parts along dimension 0
- compute_norm: bfloat16 [3072], P('job'), parts along dimension 0
- compute_bias: bfloat16 [3072], P('job'), parts along dimension 0
- stepped_up: float32 [3072, 3072], P(('job', 'dp'), 'tp'), parts along dimension 0
- stepped_down: float32 [12288, 768], P(('job', 'tp'), 'dp'), parts along dimension 0
- stepped_norm: float32 [3072], P(('job', 'dp')), parts along dimension 0
- stepped_bias: float32 [3072], P(('job', 'dp')), parts along dimension 0
- state_new_up: float32 [3072, 3072], P(('job', 'dp'), 'tp'), parts along dimension 0
- state_new_down: float32 [12288, 768], P(('job', 'tp'), 'dp'), parts along dimension 0
- state_new_norm: float32 [3072], P(('job', 'dp')), parts along dimension 0
- state_new_bias: float32 [3072], P(('job', 'dp')), parts along dimension 0
The draws below stay inside these ranges and needn't reach their ends.
There are 4 independent parts, one for each index of `job`. The reference program is written for one: setup_inputs(seed, part) draws one part's arguments, and reference() takes and returns one part's arrays. A program takes and returns all parts, laid end to end along the dimension named above; each array names one. Nothing has to cross between parts.
All inputs are finite; a program needn't handle non-finite values.
Results may differ from the reference program's by a relative error of at most 0.001.
Values may be sent and summed in bfloat16 or wider, within the bound.
A program may use at most 64 MiB of HBM per device.

```python
import jax
import jax.numpy as jnp
from jax import lax

WIDTH = 768
INNER = 3072
REPLICAS = 2


def with_spikes(values, key, source, target, shards_of, factor):
    owner, partner = [(jnp.arange(values.shape[axis_at]) // (values.shape[axis_at] // shards_of)).reshape([-1 if axis == axis_at else 1 for axis in range(values.ndim)]) for axis_at in (source, target)]
    chosen = jax.random.permutation(key, shards_of)[partner]
    strong = (owner == chosen) | (owner == (partner + shards_of // 2) % shards_of)
    return jnp.where(strong, factor * values, values)


def levels(key, shape, split, smallest, largest):
    level, own = 1.0, jax.random.fold_in(key, 6)
    for dim, parts in split:
        draws = jnp.exp(jax.random.uniform(jax.random.fold_in(own, dim), (parts,), jnp.float32, smallest / len(split), largest / len(split)))
        level = level * jnp.repeat(draws, shape[dim] // parts).reshape([-1 if axis == dim else 1 for axis in range(len(shape))])
    return level


def bell_draw(stream_key, dims, width, most, shards=(), held_as=jnp.bfloat16):
    entries = jax.random.normal(stream_key, dims, jnp.float32) * width
    if len(shards) > 0:
        entries = levels(stream_key, dims, shards, -0.22, 0.18) * entries
    return jnp.clip(entries, min=-most, max=most).astype(held_as)


def heavy_noise(rng, dims, deviation, most, cuts, heavy, kind=jnp.bfloat16):
    values = deviation * jax.random.normal(rng, dims, jnp.float32)
    if cuts:
        values = values * levels(rng, dims, cuts, -0.22, 0.18)
    return jnp.clip(with_spikes(values, jax.random.fold_in(rng, 3), *heavy), -most, most).astype(kind)


def setup_inputs(seed: int = 0, part: int = 0) -> dict:
    key_list = jax.random.split(jax.random.key(seed), 13)
    part_splits = jax.random.split(jax.random.fold_in(key_list[12], part), 13)
    return {
        "partial_up": heavy_noise(part_splits[0], (REPLICAS, WIDTH, INNER), 0.1, 0.875, ((0, 2), (2, 4)), (0, 1, 2, 2.0), jnp.float32),
        "partial_down": heavy_noise(part_splits[1], (REPLICAS, INNER, WIDTH), 0.1, 0.875, ((0, 2), (1, 4)), (0, 2, 2, 2.0), jnp.float32),
        "partial_norm": heavy_noise(part_splits[2], (REPLICAS, WIDTH), 1.0, 8.0, ((0, 2),), (0, 1, 2, 2.0), jnp.float32),
        "partial_bias": heavy_noise(part_splits[3], (REPLICAS, WIDTH), 1.0, 8.0, ((0, 2),), (0, 1, 2, 2.0), jnp.float32),
        "master_up": heavy_noise(part_splits[4], (WIDTH, INNER), WIDTH ** -0.5, 0.3125, ((0, 2), (1, 4)), (1, 0, 4, 2.0), jnp.float32),
        "master_down": heavy_noise(part_splits[5], (INNER, WIDTH), INNER ** -0.5, 0.15625, ((0, 4), (1, 2)), (0, 1, 4, 2.0), jnp.float32),
        "master_norm": jnp.clip(1.0 + 0.15 * jax.random.normal(part_splits[6], (WIDTH,), jnp.float32), 0.25, 1.75),
        "master_bias": bell_draw(part_splits[7], (WIDTH,), 0.5, 3.0, ((0, 2),), jnp.float32),
        "memory_up": bell_draw(part_splits[8], (WIDTH, INNER), WIDTH ** -0.5, 0.21875, ((0, 2), (1, 4)), jnp.float32),
        "memory_down": bell_draw(part_splits[9], (INNER, WIDTH), INNER ** -0.5, 0.109375, ((0, 4), (1, 2)), jnp.float32),
        "memory_norm": bell_draw(part_splits[10], (WIDTH,), 0.3, 1.75, ((0, 2),), jnp.float32),
        "memory_bias": bell_draw(part_splits[11], (WIDTH,), 0.3, 1.75, ((0, 2),), jnp.float32),
    }


learn_rate = 0.4
hold_rate = 0.9

def reference(partial_up, partial_down, partial_norm, partial_bias, master_up, master_down, master_norm, master_bias, memory_up, memory_down, memory_norm, memory_bias):
    mean_up = lax.optimization_barrier(jnp.sum(partial_up.astype(jnp.float32), axis=0)) * REPLICAS ** (-0.5)
    mean_down = lax.optimization_barrier(jnp.sum(partial_down.astype(jnp.float32), axis=0)) * REPLICAS ** (-0.5)
    mean_norm = lax.optimization_barrier(jnp.sum(partial_norm.astype(jnp.float32), axis=0)) * REPLICAS ** (-0.5)
    mean_bias = lax.optimization_barrier(jnp.sum(partial_bias.astype(jnp.float32), axis=0)) * REPLICAS ** (-0.5)
    ratio_up = jnp.sqrt(lax.optimization_barrier(jnp.sum(master_up * master_up, axis=1, keepdims=True))) * lax.rsqrt(lax.optimization_barrier(jnp.sum(mean_up * mean_up, axis=1, keepdims=True)) + 1e-06)
    mean_up = mean_up * ratio_up
    ratio_down = jnp.sqrt(lax.optimization_barrier(jnp.sum(master_down * master_down, axis=0, keepdims=True))) * lax.rsqrt(lax.optimization_barrier(jnp.sum(mean_down * mean_down, axis=0, keepdims=True)) + 1e-06)
    mean_down = mean_down * ratio_down
    state_new_up = hold_rate * memory_up + mean_up
    stepped_up = master_up - learn_rate * state_new_up
    state_new_down = hold_rate * memory_down + mean_down
    stepped_down = master_down - learn_rate * state_new_down
    state_new_norm = hold_rate * memory_norm + mean_norm
    stepped_norm = master_norm - learn_rate * state_new_norm
    state_new_bias = hold_rate * memory_bias + mean_bias
    stepped_bias = master_bias - learn_rate * state_new_bias
    compute_up = stepped_up.astype(jnp.bfloat16)
    compute_down = stepped_down.astype(jnp.bfloat16)
    compute_norm = stepped_norm.astype(jnp.bfloat16)
    compute_bias = stepped_bias.astype(jnp.bfloat16)
    return (compute_up, compute_down, compute_norm, compute_bias, stepped_up, stepped_down, stepped_norm, stepped_bias, state_new_up, state_new_down, state_new_norm, state_new_bias)
```

```python
import functools

import jax
import jax.numpy as jnp
from jax import lax
from jax.experimental import pallas as pl
from jax.experimental.pallas import tpu as pltpu
from jax.sharding import PartitionSpec as P

learn_rate = 0.4
hold_rate = 0.9


def on_device(
    partial_up,
    partial_down,
    partial_norm,
    partial_bias,
    master_up,
    master_down,
    master_norm,
    master_bias,
    memory_up,
    memory_down,
    memory_norm,
    memory_bias,
):
    mean_up, mean_down = (
        lax.psum_scatter(partial_up[0], "dp", scatter_dimension=0, tiled=True),
        lax.psum_scatter(partial_down[0], "dp", scatter_dimension=1, tiled=True),
    )
    whole_norm, whole_bias = lax.psum((partial_norm[0], partial_bias[0]), "dp")
    place = lax.axis_index("dp")
    mean_norm = lax.dynamic_slice_in_dim(
        whole_norm, place * master_norm.shape[0], master_norm.shape[0]
    )
    mean_bias = lax.dynamic_slice_in_dim(
        whole_bias, place * master_bias.shape[0], master_bias.shape[0]
    )
    mean_rate = lax.axis_size("dp") ** (-0.5)
    mean_up = mean_up * mean_rate
    mean_down = mean_down * mean_rate
    mean_norm = mean_norm * mean_rate
    mean_bias = mean_bias * mean_rate
    own_up, own_down, slope_up_norm, slope_down_norm = lax.psum(
        (
            jnp.sum(master_up * master_up, axis=1, keepdims=True),
            jnp.sum(master_down * master_down, axis=0, keepdims=True),
            jnp.sum(mean_up * mean_up, axis=1, keepdims=True),
            jnp.sum(mean_down * mean_down, axis=0, keepdims=True),
        ),
        "tp",
    )
    mean_up = mean_up * (jnp.sqrt(own_up) * lax.rsqrt(slope_up_norm + 1e-06))
    mean_down = mean_down * (jnp.sqrt(own_down) * lax.rsqrt(slope_down_norm + 1e-06))
    state_new_up = hold_rate * memory_up + mean_up
    stepped_up = master_up - learn_rate * state_new_up
    state_new_down = hold_rate * memory_down + mean_down
    stepped_down = master_down - learn_rate * state_new_down
    state_new_norm = hold_rate * memory_norm + mean_norm
    stepped_norm = master_norm - learn_rate * state_new_norm
    state_new_bias = hold_rate * memory_bias + mean_bias
    stepped_bias = master_bias - learn_rate * state_new_bias
    compute_up, compute_down, compute_norm, compute_bias = (
        lax.all_gather(stepped_up.astype(jnp.bfloat16), "dp", axis=0, tiled=True),
        lax.all_gather(stepped_down.astype(jnp.bfloat16), "dp", axis=1, tiled=True),
        lax.all_gather(stepped_norm.astype(jnp.bfloat16), "dp", axis=0, tiled=True),
        lax.all_gather(stepped_bias.astype(jnp.bfloat16), "dp", axis=0, tiled=True),
    )
    return (
        compute_up,
        compute_down,
        compute_norm,
        compute_bias,
        stepped_up,
        stepped_down,
        stepped_norm,
        stepped_bias,
        state_new_up,
        state_new_down,
        state_new_norm,
        state_new_bias,
    )


chunks = 4
lanes = 128


def lane_sums(x):
    total = x[:, :lanes]
    for at in range(lanes, x.shape[1], lanes):
        total = total + x[:, at : at + lanes]
    return total


def exchange(
    pu, pd, pn, pb, mu_h, md_h, mn, mb, eu_h, ed_h, en, eb,
    cu, cd, cn, cb, su, sd, sn, sb, tu, td, tn, tb,
    own_u, own_d, got_u, got_d, mu, md, eu, ed, vec, got_vec,
    sq_u, acc_d, stat_u, stat_d,
    load_sem, part_send, part_recv, vec_sem, stat_send, stat_recv, out_send, out_recv,
):
    me = lax.axis_index("dp")
    peer = 1 - me
    here = lax.axis_index("tp")
    n = lax.axis_size("tp")
    rate = lax.axis_size("dp") ** (-0.5)
    rows, wide = mu.shape
    tall, cols = md.shape
    part_u, part_d = rows // chunks, tall // chunks

    def mine(size):
        return pl.ds(pl.multiple_of(me * size, size), size)

    def theirs(size):
        return pl.ds(pl.multiple_of(peer * size, size), size)

    barrier = pltpu.get_barrier_semaphore()
    pl.semaphore_signal(barrier, inc=1, device_id={"dp": peer})
    for step in range(1, n):
        pl.semaphore_signal(barrier, inc=1, device_id={"tp": lax.rem(here + step, n)})

    loads = [
        pltpu.make_async_copy(source, target, load_sem.at[at])
        for at, (source, target) in enumerate((
            (mu_h, mu),
            (md_h, md),
            (pu.at[mine(rows), :], own_u),
            (pd.at[:, mine(cols)], own_d),
            (eu_h, eu),
            (ed_h, ed),
        ))
    ]
    for load in loads:
        load.start()

    half = mn.shape[-1]
    vec[0:1, :] = pn[...]
    vec[1:2, :] = pb[...]
    vec[2:3, :half] = mn[...].reshape(1, half)
    vec[2:3, half:] = en[...].reshape(1, half)
    vec[3:4, :half] = mb[...].reshape(1, half)
    vec[3:4, half:] = eb[...].reshape(1, half)

    pl.semaphore_wait(barrier, n)

    send_u, send_d = [], []
    for at in range(chunks):
        span = pl.ds(at * part_u, part_u)
        send_u.append(pltpu.make_async_remote_copy(
            src_ref=pu.at[pl.ds(pl.multiple_of(peer * rows + at * part_u, 8), part_u), :],
            dst_ref=got_u.at[span, :],
            send_sem=part_send.at[0, at],
            recv_sem=part_recv.at[0, at],
            device_id={"dp": peer},
        ))
        span = pl.ds(at * part_d, part_d)
        send_d.append(pltpu.make_async_remote_copy(
            src_ref=pd.at[span, theirs(cols)],
            dst_ref=got_d.at[span, :],
            send_sem=part_send.at[1, at],
            recv_sem=part_recv.at[1, at],
            device_id={"dp": peer},
        ))
    for copy in send_u + send_d:
        copy.start()
    send_vec = pltpu.make_async_remote_copy(
        src_ref=vec, dst_ref=got_vec, send_sem=vec_sem.at[0], recv_sem=vec_sem.at[1],
        device_id={"dp": peer},
    )
    send_vec.start()

    step_u, step_d = 32, 64

    loads[0].wait()

    @pl.loop(0, rows // step_u)
    def _(at):
        span = pl.ds(pl.multiple_of(at * step_u, step_u), step_u)
        x = mu[span, :]
        sq_u[span, :] = lane_sums(x * x)

    stat_u[pl.ds(here, 1), 0:1, :] = jnp.sum(sq_u[...].T, axis=0).reshape(1, 1, rows)

    def down_squares(read, start, count):
        @pl.loop(0, count // step_d)
        def _(at):
            span = pl.ds(pl.multiple_of(start + at * step_d, step_d), step_d)
            x = read(span)
            acc_d[...] += jnp.sum((x * x).reshape(step_d // 8, 8, cols), axis=0)

    loads[1].wait()
    acc_d[...] = jnp.zeros_like(acc_d)
    down_squares(lambda span: md[span, :], 0, tall)
    stat_d[pl.ds(here, 1), 0:1, :] = jnp.sum(acc_d[...], axis=0).reshape(1, 1, cols)
    acc_d[...] = jnp.zeros_like(acc_d)

    def to_peers(stat, which):
        copies = []
        for step in range(1, n):
            copies.append(pltpu.make_async_remote_copy(
                src_ref=stat.at[here],
                dst_ref=stat.at[here],
                send_sem=stat_send.at[which, step - 1],
                recv_sem=stat_recv.at[which, step - 1],
                device_id={"tp": lax.rem(here + step, n)},
            ))
        for copy in copies:
            copy.start()
        return copies

    loads[2].wait()
    for chunk in range(chunks):
        send_u[chunk].wait_recv()

        @pl.loop(0, part_u // step_u)
        def _(at):
            span = pl.ds(pl.multiple_of(chunk * part_u + at * step_u, step_u), step_u)
            x = (own_u[span, :] + got_u[span, :]) * rate
            own_u[span, :] = x
            sq_u[span, :] = lane_sums(x * x)

    stat_u[pl.ds(here, 1), 1:2, :] = jnp.sum(sq_u[...].T, axis=0).reshape(1, 1, rows)
    stats_u = to_peers(stat_u, 0)

    loads[3].wait()

    def summed(span):
        x = (own_d[span, :] + got_d[span, :]) * rate
        own_d[span, :] = x
        return x

    for chunk in range(chunks):
        send_d[chunk].wait_recv()
        down_squares(summed, chunk * part_d, part_d)
    stat_d[pl.ds(here, 1), 1:2, :] = jnp.sum(acc_d[...], axis=0).reshape(1, 1, cols)
    stats_d = to_peers(stat_d, 1)

    send_vec.wait()
    mean = (vec[0:2, :] + got_vec[0:2, :]) * rate
    for at, (state, stepped, rounded) in enumerate(((tn, sn, cn), (tb, sb, cb))):
        row = slice(2 + at, 3 + at)
        low, high = mean[at : at + 1, :half], mean[at : at + 1, half:]
        new_own = hold_rate * vec[row, half:] + jnp.where(me == 0, low, high)
        own = vec[row, :half] - learn_rate * new_own
        new_other = hold_rate * got_vec[row, half:] + jnp.where(me == 0, high, low)
        other = got_vec[row, :half] - learn_rate * new_other
        state[...] = new_own.reshape(state.shape)
        stepped[...] = own.reshape(stepped.shape)
        whole = jnp.concatenate(
            [jnp.where(me == 0, own, other), jnp.where(me == 0, other, own)], axis=1
        )
        rounded[...] = whole.reshape(rounded.shape).astype(rounded.dtype)

    def ratio_of(stat):
        total = stat[0]
        for at in range(1, n):
            total = total + stat[at]
        return jnp.sqrt(total[0:1, :]) * lax.rsqrt(total[1:2, :] + 1e-06)

    loads[4].wait()
    for copy in stats_u:
        copy.wait()
    sq_u[...] = jnp.broadcast_to(ratio_of(stat_u), (lanes, rows)).T

    out = []
    pieces = 2
    for piece in range(pieces):
        size = rows // pieces

        @pl.loop(0, size // step_u)
        def _(at):
            start = piece * size + at * step_u
            span = pl.ds(pl.multiple_of(start, step_u), step_u)
            ratio = sq_u[span, :]
            ratio = jnp.concatenate([ratio] * (wide // lanes), axis=1)
            state = hold_rate * eu[span, :] + own_u[span, :] * ratio
            stepped = mu[span, :] - learn_rate * state
            tu[span, :] = state
            su[span, :] = stepped
            place = pl.ds(pl.multiple_of(me * rows + start, step_u), step_u)
            cu[place, :] = stepped.astype(cu.dtype)

        span = pl.ds(pl.multiple_of(me * rows + piece * size, step_u), size)
        out.append(pltpu.make_async_remote_copy(
            src_ref=cu.at[span, :],
            dst_ref=cu.at[span, :],
            send_sem=out_send.at[0, piece],
            recv_sem=out_recv.at[0, piece],
            device_id={"dp": peer},
        ))
        out[-1].start()

    loads[5].wait()
    for copy in stats_d:
        copy.wait()
    ratio_d = ratio_of(stat_d)
    acc_d[...] = jnp.broadcast_to(ratio_d, acc_d.shape)
    for piece in range(pieces):
        size = tall // pieces

        @pl.loop(0, size // step_d)
        def _(at):
            span = pl.ds(pl.multiple_of(piece * size + at * step_d, step_d), step_d)
            ratio = jnp.broadcast_to(acc_d[...][None], (step_d // 8, 8, cols)).reshape(step_d, cols)
            state = hold_rate * ed[span, :] + own_d[span, :] * ratio
            stepped = md[span, :] - learn_rate * state
            td[span, :] = state
            sd[span, :] = stepped
            cd[span, mine(cols)] = stepped.astype(cd.dtype)

        span = pl.ds(piece * size, size)
        out.append(pltpu.make_async_remote_copy(
            src_ref=cd.at[span, mine(cols)],
            dst_ref=cd.at[span, mine(cols)],
            send_sem=out_send.at[1, piece],
            recv_sem=out_recv.at[1, piece],
            device_id={"dp": peer},
        ))
        out[-1].start()

    for copy in send_u + send_d:
        copy.wait_send()
    for copy in out:
        copy.wait()


def place_results(*refs):
    count = (len(refs) - 1) // 2
    sem = refs[-1]
    copies = [
        pltpu.make_async_copy(refs[at], refs[count + at], sem.at[at]) for at in range(count)
    ]
    for copy in copies:
        copy.start()
    for copy in copies:
        copy.wait()


def held(arrays):
    return [pltpu.with_memory_space_constraint(x, pltpu.HBM) for x in arrays]


def on_pair(*args):
    pu, pd, pn, pb, mu, md, mn, mb, eu, ed, en, eb = args
    n = lax.axis_size("tp")
    f32, bf16 = jnp.float32, jnp.bfloat16
    vmem = pl.BlockSpec(memory_space=pltpu.VMEM)
    hbm = pl.BlockSpec(memory_space=pltpu.HBM)
    wide, tall = pu.shape[2], pd.shape[1]
    outs = (
        ((pu.shape[1], wide), bf16),
        ((tall, pd.shape[2]), bf16),
        ((pn.shape[1],), bf16),
        ((pb.shape[1],), bf16),
        *((x.shape, f32) for x in (mu, md, mn, mb)),
        *((x.shape, f32) for x in (mu, md, mn, mb)),
    )
    rows, cols = mu.shape[0], md.shape[1]
    results = pl.pallas_call(
        exchange,
        out_shape=[jax.ShapeDtypeStruct(shape, dtype) for shape, dtype in outs],
        in_specs=[hbm, hbm, vmem, vmem, hbm, hbm, vmem, vmem, hbm, hbm, vmem, vmem],
        out_specs=[vmem] * len(outs),
        scratch_shapes=[
            pltpu.VMEM(mu.shape, f32),
            pltpu.VMEM(md.shape, f32),
            pltpu.VMEM(mu.shape, f32),
            pltpu.VMEM(md.shape, f32),
            pltpu.VMEM(mu.shape, f32),
            pltpu.VMEM(md.shape, f32),
            pltpu.VMEM(mu.shape, f32),
            pltpu.VMEM(md.shape, f32),
            pltpu.VMEM((4, pn.shape[1]), f32),
            pltpu.VMEM((4, pn.shape[1]), f32),
            pltpu.VMEM((rows, lanes), f32),
            pltpu.VMEM((8, cols), f32),
            pltpu.VMEM((n, 2, rows), f32),
            pltpu.VMEM((n, 2, cols), f32),
            pltpu.SemaphoreType.DMA((6,)),
            pltpu.SemaphoreType.DMA((2, chunks)),
            pltpu.SemaphoreType.DMA((2, chunks)),
            pltpu.SemaphoreType.DMA((2,)),
            pltpu.SemaphoreType.DMA((2, n - 1)),
            pltpu.SemaphoreType.DMA((2, n - 1)),
            pltpu.SemaphoreType.DMA((2, 2)),
            pltpu.SemaphoreType.DMA((2, 2)),
        ],
        compiler_params=pltpu.CompilerParams(
            collective_id=0, has_side_effects=True, vmem_limit_bytes=40 * 2**20
        ),
        name="exchange",
    )(*held((pu[0], pd[0])), pn, pb, *held((mu, md)), mn, mb, *held((eu, ed)), en, eb)
    return tuple(pl.pallas_call(
        place_results,
        out_shape=[jax.ShapeDtypeStruct(shape, dtype) for shape, dtype in outs],
        in_specs=[vmem] * len(outs),
        out_specs=[hbm] * len(outs),
        scratch_shapes=[pltpu.SemaphoreType.DMA((len(outs),))],
        compiler_params=pltpu.CompilerParams(vmem_limit_bytes=2**20),
        name="place_results",
    )(*results))


def solution(mesh):
    in_specs = (
        P(("job", "dp"), None, "tp"),
        P(("job", "dp"), "tp", None),
        P(("job", "dp"), None),
        P(("job", "dp"), None),
        P(("job", "dp"), "tp"),
        P(("job", "tp"), "dp"),
        P(("job", "dp")),
        P(("job", "dp")),
        P(("job", "dp"), "tp"),
        P(("job", "tp"), "dp"),
        P(("job", "dp")),
        P(("job", "dp")),
    )
    out_specs = (
        P("job", "tp"),
        P(("job", "tp"), None),
        P("job"),
        P("job"),
        P(("job", "dp"), "tp"),
        P(("job", "tp"), "dp"),
        P(("job", "dp")),
        P(("job", "dp")),
        P(("job", "dp"), "tp"),
        P(("job", "tp"), "dp"),
        P(("job", "dp")),
        P(("job", "dp")),
    )
    return jax.shard_map(
        on_device if mesh.shape["dp"] != 2 else on_pair, mesh=mesh, in_specs=in_specs, out_specs=out_specs, check_vma=False
    )
```

```python
import functools

import jax
import jax.numpy as jnp
from jax import lax
from jax.experimental import pallas as pl
from jax.experimental.pallas import tpu as pltpu
from jax.sharding import PartitionSpec as P

learn_rate = 0.4
hold_rate = 0.9


def on_device(
    partial_up,
    partial_down,
    partial_norm,
    partial_bias,
    master_up,
    master_down,
    master_norm,
    master_bias,
    memory_up,
    memory_down,
    memory_norm,
    memory_bias,
):
    mean_up, mean_down = (
        lax.psum_scatter(partial_up[0], "dp", scatter_dimension=0, tiled=True),
        lax.psum_scatter(partial_down[0], "dp", scatter_dimension=1, tiled=True),
    )
    whole_norm, whole_bias = lax.psum((partial_norm[0], partial_bias[0]), "dp")
    place = lax.axis_index("dp")
    mean_norm = lax.dynamic_slice_in_dim(
        whole_norm, place * master_norm.shape[0], master_norm.shape[0]
    )
    mean_bias = lax.dynamic_slice_in_dim(
        whole_bias, place * master_bias.shape[0], master_bias.shape[0]
    )
    mean_rate = lax.axis_size("dp") ** (-0.5)
    mean_up = mean_up * mean_rate
    mean_down = mean_down * mean_rate
    mean_norm = mean_norm * mean_rate
    mean_bias = mean_bias * mean_rate
    own_up, own_down, slope_up_norm, slope_down_norm = lax.psum(
        (
            jnp.sum(master_up * master_up, axis=1, keepdims=True),
            jnp.sum(master_down * master_down, axis=0, keepdims=True),
            jnp.sum(mean_up * mean_up, axis=1, keepdims=True),
            jnp.sum(mean_down * mean_down, axis=0, keepdims=True),
        ),
        "tp",
    )
    mean_up = mean_up * (jnp.sqrt(own_up) * lax.rsqrt(slope_up_norm + 1e-06))
    mean_down = mean_down * (jnp.sqrt(own_down) * lax.rsqrt(slope_down_norm + 1e-06))
    state_new_up = hold_rate * memory_up + mean_up
    stepped_up = master_up - learn_rate * state_new_up
    state_new_down = hold_rate * memory_down + mean_down
    stepped_down = master_down - learn_rate * state_new_down
    state_new_norm = hold_rate * memory_norm + mean_norm
    stepped_norm = master_norm - learn_rate * state_new_norm
    state_new_bias = hold_rate * memory_bias + mean_bias
    stepped_bias = master_bias - learn_rate * state_new_bias
    compute_up, compute_down, compute_norm, compute_bias = (
        lax.all_gather(stepped_up.astype(jnp.bfloat16), "dp", axis=0, tiled=True),
        lax.all_gather(stepped_down.astype(jnp.bfloat16), "dp", axis=1, tiled=True),
        lax.all_gather(stepped_norm.astype(jnp.bfloat16), "dp", axis=0, tiled=True),
        lax.all_gather(stepped_bias.astype(jnp.bfloat16), "dp", axis=0, tiled=True),
    )
    return (
        compute_up,
        compute_down,
        compute_norm,
        compute_bias,
        stepped_up,
        stepped_down,
        stepped_norm,
        stepped_bias,
        state_new_up,
        state_new_down,
        state_new_norm,
        state_new_bias,
    )


chunks = 4
pieces = 4
lanes = 128


def lane_sums(x):
    total = x[:, :lanes]
    for at in range(lanes, x.shape[1], lanes):
        total = total + x[:, at : at + lanes]
    return total


def exchange(
    pu, pd, pn, pb, mu_h, md_h, mn, mb, eu_h, ed_h, en, eb,
    cu, cd, cn, cb, su, sd, sn, sb, tu, td, tn, tb,
    own_u, own_d, give_u, give_d, got_u, got_d, mu, md, eu, ed, pn_v, pb_v, mn_v, mb_v, en_v, eb_v, vec, got_vec,
    sq_u, acc_d, stat_u, stat_d,
    load_sem, give_sem, knows, part_send, part_recv, vec_sem, stat_send, stat_recv, out_send, out_recv,
):
    me = lax.axis_index("dp")
    peer = 1 - me
    here = lax.axis_index("tp")
    n = lax.axis_size("tp")
    rate = lax.axis_size("dp") ** (-0.5)
    rows, wide = mu.shape
    tall, cols = md.shape
    part_u, part_d = rows // chunks, tall // chunks

    def mine(size):
        return pl.ds(pl.multiple_of(me * size, size), size)

    def theirs(size):
        return pl.ds(pl.multiple_of(peer * size, size), size)

    has_left, has_right = here > 0, here < n - 1

    def to_neighbours(left_sem, right_sem):
        @pl.when(has_left)
        def _():
            pl.semaphore_signal(left_sem, inc=1, device_id={"tp": here - 1})

        @pl.when(has_right)
        def _():
            pl.semaphore_signal(right_sem, inc=1, device_id={"tp": here + 1})

    barrier = pltpu.get_barrier_semaphore()
    pl.semaphore_signal(barrier, inc=1, device_id={"dp": peer})
    to_neighbours(barrier, barrier)

    give = []
    for at in range(chunks):
        span = pl.ds(at * part_u, part_u)
        give.append(pltpu.make_async_copy(
            pu.at[pl.ds(pl.multiple_of(peer * rows + at * part_u, 8), part_u), :],
            give_u.at[span, :],
            give_sem.at[0, at],
        ))
    for at in range(chunks):
        span = pl.ds(at * part_d, part_d)
        give.append(pltpu.make_async_copy(
            pd.at[span, theirs(cols)], give_d.at[span, :], give_sem.at[1, at]
        ))
    loads = [
        pltpu.make_async_copy(source, target, load_sem.at[at])
        for at, (source, target) in enumerate((
            (mu_h, mu),
            (md_h, md),
            (pu.at[mine(rows), :], own_u),
            (pd.at[:, mine(cols)], own_d),
            (eu_h, eu),
            (ed_h, ed),
            (pn, pn_v),
            (pb, pb_v),
            (mn, mn_v),
            (mb, mb_v),
            (en, en_v),
            (eb, eb_v),
        ))
    ]
    for load in give + loads[6:] + loads[:6]:
        load.start()

    pl.semaphore_wait(barrier, 1 + has_left.astype(jnp.int32) + has_right.astype(jnp.int32))

    send_u, send_d = [], []
    for at in range(chunks):
        span = pl.ds(at * part_u, part_u)
        send_u.append(pltpu.make_async_remote_copy(
            src_ref=give_u.at[span, :],
            dst_ref=got_u.at[span, :],
            send_sem=part_send.at[0, at],
            recv_sem=part_recv.at[0, at],
            device_id={"dp": peer},
        ))
        span = pl.ds(at * part_d, part_d)
        send_d.append(pltpu.make_async_remote_copy(
            src_ref=give_d.at[span, :],
            dst_ref=got_d.at[span, :],
            send_sem=part_send.at[1, at],
            recv_sem=part_recv.at[1, at],
            device_id={"dp": peer},
        ))
    for load, copy in zip(give, send_u + send_d):
        load.wait()
        copy.start()
    if n > 2:
        to_neighbours(knows.at[0], knows.at[1])

    half = mn.shape[-1]
    for load in loads[6:]:
        load.wait()
    vec[0:1, :] = pn_v[...]
    vec[1:2, :] = pb_v[...]
    vec[2:3, :half] = mn_v[...].reshape(1, half)
    vec[2:3, half:] = en_v[...].reshape(1, half)
    vec[3:4, :half] = mb_v[...].reshape(1, half)
    vec[3:4, half:] = eb_v[...].reshape(1, half)

    step_u, step_d = 32, 64

    loads[0].wait()

    @pl.loop(0, rows // step_u)
    def _(at):
        span = pl.ds(pl.multiple_of(at * step_u, step_u), step_u)
        x = mu[span, :]
        sq_u[span, :] = lane_sums(x * x)

    stat_u[pl.ds(here, 1), 0:1, :] = jnp.sum(sq_u[...].T, axis=0).reshape(1, 1, rows)

    def down_squares(read, start, count):
        @pl.loop(0, count // step_d)
        def _(at):
            span = pl.ds(pl.multiple_of(start + at * step_d, step_d), step_d)
            x = read(span)
            acc_d[...] += jnp.sum((x * x).reshape(step_d // 8, 8, cols), axis=0)

    send_vec = pltpu.make_async_remote_copy(
        src_ref=vec, dst_ref=got_vec, send_sem=vec_sem.at[0], recv_sem=vec_sem.at[1],
        device_id={"dp": peer},
    )
    send_vec.start()

    def hear():
        @pl.when(has_right)
        def _():
            pl.semaphore_wait(knows.at[0], 1)

        @pl.when(has_left)
        def _():
            pl.semaphore_wait(knows.at[1], 1)

    loads[1].wait()
    acc_d[...] = jnp.zeros_like(acc_d)
    down_squares(lambda span: md[span, :], 0, tall)
    stat_d[pl.ds(here, 1), 0:1, :] = jnp.sum(acc_d[...], axis=0).reshape(1, 1, cols)
    acc_d[...] = jnp.zeros_like(acc_d)
    for reach in range(2, n):
        hear()
        if reach < n - 1:
            to_neighbours(knows.at[0], knows.at[1])

    def to_peers(stat, which):
        copies = []
        for step in range(1, n):
            copies.append(pltpu.make_async_remote_copy(
                src_ref=stat.at[here],
                dst_ref=stat.at[here],
                send_sem=stat_send.at[which, step - 1],
                recv_sem=stat_recv.at[which, step - 1],
                device_id={"tp": lax.rem(here + step, n)},
            ))
        for copy in copies:
            copy.start()
        return copies

    loads[2].wait()
    for chunk in range(chunks):
        send_u[chunk].wait_recv()

        @pl.loop(0, part_u // step_u)
        def _(at):
            span = pl.ds(pl.multiple_of(chunk * part_u + at * step_u, step_u), step_u)
            x = (own_u[span, :] + got_u[span, :]) * rate
            own_u[span, :] = x
            sq_u[span, :] = lane_sums(x * x)

    stat_u[pl.ds(here, 1), 1:2, :] = jnp.sum(sq_u[...].T, axis=0).reshape(1, 1, rows)
    stats_u = to_peers(stat_u, 0)

    loads[3].wait()

    def summed(span):
        x = (own_d[span, :] + got_d[span, :]) * rate
        own_d[span, :] = x
        return x

    for chunk in range(chunks):
        send_d[chunk].wait_recv()
        down_squares(summed, chunk * part_d, part_d)
    stat_d[pl.ds(here, 1), 1:2, :] = jnp.sum(acc_d[...], axis=0).reshape(1, 1, cols)
    stats_d = to_peers(stat_d, 1)

    send_vec.wait()
    mean = (vec[0:2, :] + got_vec[0:2, :]) * rate
    for at, (state, stepped, rounded) in enumerate(((tn, sn, cn), (tb, sb, cb))):
        row = slice(2 + at, 3 + at)
        low, high = mean[at : at + 1, :half], mean[at : at + 1, half:]
        new_own = hold_rate * vec[row, half:] + jnp.where(me == 0, low, high)
        own = vec[row, :half] - learn_rate * new_own
        new_other = hold_rate * got_vec[row, half:] + jnp.where(me == 0, high, low)
        other = got_vec[row, :half] - learn_rate * new_other
        state[...] = new_own.reshape(state.shape)
        stepped[...] = own.reshape(stepped.shape)
        whole = jnp.concatenate(
            [jnp.where(me == 0, own, other), jnp.where(me == 0, other, own)], axis=1
        )
        rounded[...] = whole.reshape(rounded.shape).astype(rounded.dtype)

    def ratio_of(stat):
        total = stat[0]
        for at in range(1, n):
            total = total + stat[at]
        return jnp.sqrt(total[0:1, :]) * lax.rsqrt(total[1:2, :] + 1e-06)

    loads[4].wait()
    for copy in stats_u:
        copy.wait()
    sq_u[...] = jnp.broadcast_to(ratio_of(stat_u), (lanes, rows)).T

    out = []
    for piece in range(pieces):
        size = rows // pieces

        @pl.loop(0, size // step_u)
        def _(at):
            start = piece * size + at * step_u
            span = pl.ds(pl.multiple_of(start, step_u), step_u)
            ratio = sq_u[span, :]
            ratio = jnp.concatenate([ratio] * (wide // lanes), axis=1)
            state = hold_rate * eu[span, :] + own_u[span, :] * ratio
            stepped = mu[span, :] - learn_rate * state
            tu[span, :] = state
            su[span, :] = stepped
            place = pl.ds(pl.multiple_of(me * rows + start, step_u), step_u)
            cu[place, :] = stepped.astype(cu.dtype)

        span = pl.ds(pl.multiple_of(me * rows + piece * size, step_u), size)
        out.append(pltpu.make_async_remote_copy(
            src_ref=cu.at[span, :],
            dst_ref=cu.at[span, :],
            send_sem=out_send.at[0, piece],
            recv_sem=out_recv.at[0, piece],
            device_id={"dp": peer},
        ))
        out[-1].start()

    loads[5].wait()
    for copy in stats_d:
        copy.wait()
    ratio_d = ratio_of(stat_d)
    acc_d[...] = jnp.broadcast_to(ratio_d, acc_d.shape)
    for piece in range(pieces):
        size = tall // pieces

        @pl.loop(0, size // step_d)
        def _(at):
            span = pl.ds(pl.multiple_of(piece * size + at * step_d, step_d), step_d)
            ratio = jnp.broadcast_to(acc_d[...][None], (step_d // 8, 8, cols)).reshape(step_d, cols)
            state = hold_rate * ed[span, :] + own_d[span, :] * ratio
            stepped = md[span, :] - learn_rate * state
            td[span, :] = state
            sd[span, :] = stepped
            cd[span, mine(cols)] = stepped.astype(cd.dtype)

        span = pl.ds(piece * size, size)
        out.append(pltpu.make_async_remote_copy(
            src_ref=cd.at[span, mine(cols)],
            dst_ref=cd.at[span, mine(cols)],
            send_sem=out_send.at[1, piece],
            recv_sem=out_recv.at[1, piece],
            device_id={"dp": peer},
        ))
        out[-1].start()

    for copy in send_u + send_d:
        copy.wait_send()
    for copy in out:
        copy.wait()


def place_results(*refs):
    count = (len(refs) - 1) // 2
    sem = refs[-1]
    copies = []
    for at in range(count):
        source, target = refs[at], refs[count + at]
        if len(source.shape) == 1:
            copies.append(pltpu.make_async_copy(source, target, sem.at[at, 0]))
            continue
        size = source.shape[0] // pieces
        for piece in range(pieces):
            span = pl.ds(piece * size, size)
            copies.append(pltpu.make_async_copy(
                source.at[span, :], target.at[span, :], sem.at[at, piece]
            ))
    for copy in copies:
        copy.start()
    for copy in copies:
        copy.wait()


def held(arrays):
    return [pltpu.with_memory_space_constraint(x, pltpu.HBM) for x in arrays]


def on_pair(*args):
    pu, pd, pn, pb, mu, md, mn, mb, eu, ed, en, eb = args
    n = lax.axis_size("tp")
    f32, bf16 = jnp.float32, jnp.bfloat16
    vmem = pl.BlockSpec(memory_space=pltpu.VMEM)
    hbm = pl.BlockSpec(memory_space=pltpu.HBM)
    wide, tall = pu.shape[2], pd.shape[1]
    outs = (
        ((pu.shape[1], wide), bf16),
        ((tall, pd.shape[2]), bf16),
        ((pn.shape[1],), bf16),
        ((pb.shape[1],), bf16),
        *((x.shape, f32) for x in (mu, md, mn, mb)),
        *((x.shape, f32) for x in (mu, md, mn, mb)),
    )
    rows, cols = mu.shape[0], md.shape[1]
    results = pl.pallas_call(
        exchange,
        out_shape=[jax.ShapeDtypeStruct(shape, dtype) for shape, dtype in outs],
        in_specs=[hbm] * len(args),
        out_specs=[vmem] * len(outs),
        scratch_shapes=[
            *(pltpu.VMEM(x.shape, f32) for x in (mu, md) * 5),
            *(pltpu.VMEM(x.shape, f32) for x in (pn, pb, mn, mb, en, eb)),
            pltpu.VMEM((4, pn.shape[1]), f32),
            pltpu.VMEM((4, pn.shape[1]), f32),
            pltpu.VMEM((rows, lanes), f32),
            pltpu.VMEM((8, cols), f32),
            pltpu.VMEM((n, 2, rows), f32),
            pltpu.VMEM((n, 2, cols), f32),
            pltpu.SemaphoreType.DMA((12,)),
            pltpu.SemaphoreType.DMA((2, chunks)),
            pltpu.SemaphoreType.REGULAR((2,)),
            pltpu.SemaphoreType.DMA((2, chunks)),
            pltpu.SemaphoreType.DMA((2, chunks)),
            pltpu.SemaphoreType.DMA((2,)),
            pltpu.SemaphoreType.DMA((2, n - 1)),
            pltpu.SemaphoreType.DMA((2, n - 1)),
            pltpu.SemaphoreType.DMA((2, pieces)),
            pltpu.SemaphoreType.DMA((2, pieces)),
        ],
        compiler_params=pltpu.CompilerParams(
            collective_id=0, has_side_effects=True, vmem_limit_bytes=40 * 2**20
        ),
        name="exchange",
    )(*held((pu[0], pd[0], *args[2:])))
    return tuple(pl.pallas_call(
        place_results,
        out_shape=[jax.ShapeDtypeStruct(shape, dtype) for shape, dtype in outs],
        in_specs=[vmem] * len(outs),
        out_specs=[hbm] * len(outs),
        scratch_shapes=[pltpu.SemaphoreType.DMA((len(outs), pieces))],
        compiler_params=pltpu.CompilerParams(vmem_limit_bytes=2**20),
        name="place_results",
    )(*results))


def solution(mesh):
    in_specs = (
        P(("job", "dp"), None, "tp"),
        P(("job", "dp"), "tp", None),
        P(("job", "dp"), None),
        P(("job", "dp"), None),
        P(("job", "dp"), "tp"),
        P(("job", "tp"), "dp"),
        P(("job", "dp")),
        P(("job", "dp")),
        P(("job", "dp"), "tp"),
        P(("job", "tp"), "dp"),
        P(("job", "dp")),
        P(("job", "dp")),
    )
    out_specs = (
        P("job", "tp"),
        P(("job", "tp"), None),
        P("job"),
        P("job"),
        P(("job", "dp"), "tp"),
        P(("job", "tp"), "dp"),
        P(("job", "dp")),
        P(("job", "dp")),
        P(("job", "dp"), "tp"),
        P(("job", "tp"), "dp"),
        P(("job", "dp")),
        P(("job", "dp")),
    )
    return jax.shard_map(
        on_device if mesh.shape["dp"] != 2 else on_pair, mesh=mesh, in_specs=in_specs, out_specs=out_specs, check_vma=False
    )
```

```python
import functools

import jax
import jax.numpy as jnp
from jax import lax
from jax.experimental import pallas as pl
from jax.experimental.pallas import tpu as pltpu
from jax.sharding import PartitionSpec as P

learn_rate = 0.4
hold_rate = 0.9


def on_device(
    partial_up,
    partial_down,
    partial_norm,
    partial_bias,
    master_up,
    master_down,
    master_norm,
    master_bias,
    memory_up,
    memory_down,
    memory_norm,
    memory_bias,
):
    mean_up, mean_down = (
        lax.psum_scatter(partial_up[0], "dp", scatter_dimension=0, tiled=True),
        lax.psum_scatter(partial_down[0], "dp", scatter_dimension=1, tiled=True),
    )
    whole_norm, whole_bias = lax.psum((partial_norm[0], partial_bias[0]), "dp")
    place = lax.axis_index("dp")
    mean_norm = lax.dynamic_slice_in_dim(
        whole_norm, place * master_norm.shape[0], master_norm.shape[0]
    )
    mean_bias = lax.dynamic_slice_in_dim(
        whole_bias, place * master_bias.shape[0], master_bias.shape[0]
    )
    mean_rate = lax.axis_size("dp") ** (-0.5)
    mean_up = mean_up * mean_rate
    mean_down = mean_down * mean_rate
    mean_norm = mean_norm * mean_rate
    mean_bias = mean_bias * mean_rate
    own_up, own_down, slope_up_norm, slope_down_norm = lax.psum(
        (
            jnp.sum(master_up * master_up, axis=1, keepdims=True),
            jnp.sum(master_down * master_down, axis=0, keepdims=True),
            jnp.sum(mean_up * mean_up, axis=1, keepdims=True),
            jnp.sum(mean_down * mean_down, axis=0, keepdims=True),
        ),
        "tp",
    )
    mean_up = mean_up * (jnp.sqrt(own_up) * lax.rsqrt(slope_up_norm + 1e-06))
    mean_down = mean_down * (jnp.sqrt(own_down) * lax.rsqrt(slope_down_norm + 1e-06))
    state_new_up = hold_rate * memory_up + mean_up
    stepped_up = master_up - learn_rate * state_new_up
    state_new_down = hold_rate * memory_down + mean_down
    stepped_down = master_down - learn_rate * state_new_down
    state_new_norm = hold_rate * memory_norm + mean_norm
    stepped_norm = master_norm - learn_rate * state_new_norm
    state_new_bias = hold_rate * memory_bias + mean_bias
    stepped_bias = master_bias - learn_rate * state_new_bias
    compute_up, compute_down, compute_norm, compute_bias = (
        lax.all_gather(stepped_up.astype(jnp.bfloat16), "dp", axis=0, tiled=True),
        lax.all_gather(stepped_down.astype(jnp.bfloat16), "dp", axis=1, tiled=True),
        lax.all_gather(stepped_norm.astype(jnp.bfloat16), "dp", axis=0, tiled=True),
        lax.all_gather(stepped_bias.astype(jnp.bfloat16), "dp", axis=0, tiled=True),
    )
    return (
        compute_up,
        compute_down,
        compute_norm,
        compute_bias,
        stepped_up,
        stepped_down,
        stepped_norm,
        stepped_bias,
        state_new_up,
        state_new_down,
        state_new_norm,
        state_new_bias,
    )


chunks = 4
pieces = 4
lanes = 128


def lane_sums(x):
    total = x[:, :lanes]
    for at in range(lanes, x.shape[1], lanes):
        total = total + x[:, at : at + lanes]
    return total


def exchange(
    pu, pd, pn, pb, mu_h, md_h, mn, mb, eu_h, ed_h, en, eb,
    cu, cd, cn, cb, su, sd, sn, sb, tu, td, tn, tb,
    own_u, own_d, give_u, give_d, got_u, got_d, mu, md, eu, ed, pn_v, pb_v, mn_v, mb_v, en_v, eb_v, vec, got_vec,
    sq_u, acc_d, stat_u, stat_d,
    load_sem, give_sem, part_send, part_recv, vec_sem, stat_send, stat_recv, out_send, out_recv,
):
    me = lax.axis_index("dp")
    peer = 1 - me
    here = lax.axis_index("tp")
    n = lax.axis_size("tp")
    rate = lax.axis_size("dp") ** (-0.5)
    rows, wide = mu.shape
    tall, cols = md.shape
    part_u, part_d = rows // chunks, tall // chunks

    def mine(size):
        return pl.ds(pl.multiple_of(me * size, size), size)

    def theirs(size):
        return pl.ds(pl.multiple_of(peer * size, size), size)

    barrier = pltpu.get_barrier_semaphore()
    pl.semaphore_signal(barrier, inc=1, device_id={"dp": peer})
    for step in range(1, n):
        pl.semaphore_signal(barrier, inc=1, device_id={"tp": lax.rem(here + step, n)})

    give = []
    for at in range(chunks):
        span = pl.ds(at * part_u, part_u)
        give.append(pltpu.make_async_copy(
            pu.at[pl.ds(pl.multiple_of(peer * rows + at * part_u, 8), part_u), :],
            give_u.at[span, :],
            give_sem.at[0, at],
        ))
    for at in range(chunks):
        span = pl.ds(at * part_d, part_d)
        give.append(pltpu.make_async_copy(
            pd.at[span, theirs(cols)], give_d.at[span, :], give_sem.at[1, at]
        ))
    loads = [
        pltpu.make_async_copy(source, target, load_sem.at[at])
        for at, (source, target) in enumerate((
            (mu_h, mu),
            (md_h, md),
            (pu.at[mine(rows), :], own_u),
            (pd.at[:, mine(cols)], own_d),
            (eu_h, eu),
            (ed_h, ed),
            (pn, pn_v),
            (pb, pb_v),
            (mn, mn_v),
            (mb, mb_v),
            (en, en_v),
            (eb, eb_v),
        ))
    ]

    pl.semaphore_wait(barrier, n)

    send_u, send_d = [], []
    for at in range(chunks):
        span = pl.ds(at * part_u, part_u)
        send_u.append(pltpu.make_async_remote_copy(
            src_ref=pu.at[pl.ds(pl.multiple_of(peer * rows + at * part_u, 8), part_u), :],
            dst_ref=got_u.at[span, :],
            send_sem=part_send.at[0, at],
            recv_sem=part_recv.at[0, at],
            device_id={"dp": peer},
        ))
        span = pl.ds(at * part_d, part_d)
        send_d.append(pltpu.make_async_remote_copy(
            src_ref=pd.at[span, theirs(cols)],
            dst_ref=got_d.at[span, :],
            send_sem=part_send.at[1, at],
            recv_sem=part_recv.at[1, at],
            device_id={"dp": peer},
        ))
    for load, copy in zip(give[:chunks], send_u):
        copy.start()
    for load in (loads[0], loads[2], *loads[6:]):
        load.start()
    for load, copy in zip(give[chunks:], send_d):
        copy.start()
    for load in (loads[1], *loads[3:6]):
        load.start()

    half = mn.shape[-1]
    for load in loads[6:]:
        load.wait()
    vec[0:1, :] = pn_v[...]
    vec[1:2, :] = pb_v[...]
    vec[2:3, :half] = mn_v[...].reshape(1, half)
    vec[2:3, half:] = en_v[...].reshape(1, half)
    vec[3:4, :half] = mb_v[...].reshape(1, half)
    vec[3:4, half:] = eb_v[...].reshape(1, half)

    step_u, step_d = 32, 64

    loads[0].wait()

    @pl.loop(0, rows // step_u)
    def _(at):
        span = pl.ds(pl.multiple_of(at * step_u, step_u), step_u)
        x = mu[span, :]
        sq_u[span, :] = lane_sums(x * x)

    stat_u[pl.ds(here, 1), 0:1, :] = jnp.sum(sq_u[...].T, axis=0).reshape(1, 1, rows)

    def down_squares(read, start, count):
        @pl.loop(0, count // step_d)
        def _(at):
            span = pl.ds(pl.multiple_of(start + at * step_d, step_d), step_d)
            x = read(span)
            acc_d[...] += jnp.sum((x * x).reshape(step_d // 8, 8, cols), axis=0)

    send_vec = pltpu.make_async_remote_copy(
        src_ref=vec, dst_ref=got_vec, send_sem=vec_sem.at[0], recv_sem=vec_sem.at[1],
        device_id={"dp": peer},
    )
    send_vec.start()

    loads[1].wait()
    acc_d[...] = jnp.zeros_like(acc_d)
    down_squares(lambda span: md[span, :], 0, tall)
    stat_d[pl.ds(here, 1), 0:1, :] = jnp.sum(acc_d[...], axis=0).reshape(1, 1, cols)
    acc_d[...] = jnp.zeros_like(acc_d)

    def to_peers(stat, which):
        copies = []
        for step in range(1, n):
            copies.append(pltpu.make_async_remote_copy(
                src_ref=stat.at[here],
                dst_ref=stat.at[here],
                send_sem=stat_send.at[which, step - 1],
                recv_sem=stat_recv.at[which, step - 1],
                device_id={"tp": lax.rem(here + step, n)},
            ))
        for copy in copies:
            copy.start()
        return copies

    loads[2].wait()
    for chunk in range(chunks):
        send_u[chunk].wait_recv()

        @pl.loop(0, part_u // step_u)
        def _(at):
            span = pl.ds(pl.multiple_of(chunk * part_u + at * step_u, step_u), step_u)
            x = (own_u[span, :] + got_u[span, :]) * rate
            own_u[span, :] = x
            sq_u[span, :] = lane_sums(x * x)

    stat_u[pl.ds(here, 1), 1:2, :] = jnp.sum(sq_u[...].T, axis=0).reshape(1, 1, rows)
    stats_u = to_peers(stat_u, 0)

    loads[3].wait()

    def summed(span):
        x = (own_d[span, :] + got_d[span, :]) * rate
        own_d[span, :] = x
        return x

    for chunk in range(chunks):
        send_d[chunk].wait_recv()
        down_squares(summed, chunk * part_d, part_d)
    stat_d[pl.ds(here, 1), 1:2, :] = jnp.sum(acc_d[...], axis=0).reshape(1, 1, cols)
    stats_d = to_peers(stat_d, 1)

    send_vec.wait()
    mean = (vec[0:2, :] + got_vec[0:2, :]) * rate
    for at, (state, stepped, rounded) in enumerate(((tn, sn, cn), (tb, sb, cb))):
        row = slice(2 + at, 3 + at)
        low, high = mean[at : at + 1, :half], mean[at : at + 1, half:]
        new_own = hold_rate * vec[row, half:] + jnp.where(me == 0, low, high)
        own = vec[row, :half] - learn_rate * new_own
        new_other = hold_rate * got_vec[row, half:] + jnp.where(me == 0, high, low)
        other = got_vec[row, :half] - learn_rate * new_other
        state[...] = new_own.reshape(state.shape)
        stepped[...] = own.reshape(stepped.shape)
        whole = jnp.concatenate(
            [jnp.where(me == 0, own, other), jnp.where(me == 0, other, own)], axis=1
        )
        rounded[...] = whole.reshape(rounded.shape).astype(rounded.dtype)

    def ratio_of(stat):
        total = stat[0]
        for at in range(1, n):
            total = total + stat[at]
        return jnp.sqrt(total[0:1, :]) * lax.rsqrt(total[1:2, :] + 1e-06)

    loads[4].wait()
    for copy in stats_u:
        copy.wait()
    sq_u[...] = jnp.broadcast_to(ratio_of(stat_u), (lanes, rows)).T

    out = []
    for piece in range(pieces):
        size = rows // pieces

        @pl.loop(0, size // step_u)
        def _(at):
            start = piece * size + at * step_u
            span = pl.ds(pl.multiple_of(start, step_u), step_u)
            ratio = sq_u[span, :]
            ratio = jnp.concatenate([ratio] * (wide // lanes), axis=1)
            state = hold_rate * eu[span, :] + own_u[span, :] * ratio
            stepped = mu[span, :] - learn_rate * state
            tu[span, :] = state
            su[span, :] = stepped
            place = pl.ds(pl.multiple_of(me * rows + start, step_u), step_u)
            cu[place, :] = stepped.astype(cu.dtype)

        span = pl.ds(pl.multiple_of(me * rows + piece * size, step_u), size)
        out.append(pltpu.make_async_remote_copy(
            src_ref=cu.at[span, :],
            dst_ref=cu.at[span, :],
            send_sem=out_send.at[0, piece],
            recv_sem=out_recv.at[0, piece],
            device_id={"dp": peer},
        ))
        out[-1].start()

    loads[5].wait()
    for copy in stats_d:
        copy.wait()
    ratio_d = ratio_of(stat_d)
    acc_d[...] = jnp.broadcast_to(ratio_d, acc_d.shape)
    for piece in range(pieces):
        size = tall // pieces

        @pl.loop(0, size // step_d)
        def _(at):
            span = pl.ds(pl.multiple_of(piece * size + at * step_d, step_d), step_d)
            ratio = jnp.broadcast_to(acc_d[...][None], (step_d // 8, 8, cols)).reshape(step_d, cols)
            state = hold_rate * ed[span, :] + own_d[span, :] * ratio
            stepped = md[span, :] - learn_rate * state
            td[span, :] = state
            sd[span, :] = stepped
            cd[span, mine(cols)] = stepped.astype(cd.dtype)

        span = pl.ds(piece * size, size)
        out.append(pltpu.make_async_remote_copy(
            src_ref=cd.at[span, mine(cols)],
            dst_ref=cd.at[span, mine(cols)],
            send_sem=out_send.at[1, piece],
            recv_sem=out_recv.at[1, piece],
            device_id={"dp": peer},
        ))
        out[-1].start()

    for copy in send_u + send_d:
        copy.wait_send()
    for copy in out:
        copy.wait()


def place_results(*refs):
    count = (len(refs) - 1) // 2
    sem = refs[-1]
    copies = [
        pltpu.make_async_copy(refs[at], refs[count + at], sem.at[at]) for at in range(count)
    ]
    for copy in copies:
        copy.start()
    for copy in copies:
        copy.wait()


def held(arrays):
    return [pltpu.with_memory_space_constraint(x, pltpu.HBM) for x in arrays]


def on_pair(*args):
    pu, pd, pn, pb, mu, md, mn, mb, eu, ed, en, eb = args
    n = lax.axis_size("tp")
    f32, bf16 = jnp.float32, jnp.bfloat16
    vmem = pl.BlockSpec(memory_space=pltpu.VMEM)
    hbm = pl.BlockSpec(memory_space=pltpu.HBM)
    wide, tall = pu.shape[2], pd.shape[1]
    outs = (
        ((pu.shape[1], wide), bf16),
        ((tall, pd.shape[2]), bf16),
        ((pn.shape[1],), bf16),
        ((pb.shape[1],), bf16),
        *((x.shape, f32) for x in (mu, md, mn, mb)),
        *((x.shape, f32) for x in (mu, md, mn, mb)),
    )
    rows, cols = mu.shape[0], md.shape[1]
    results = pl.pallas_call(
        exchange,
        out_shape=[jax.ShapeDtypeStruct(shape, dtype) for shape, dtype in outs],
        in_specs=[hbm] * len(args),
        out_specs=[vmem] * len(outs),
        scratch_shapes=[
            *(pltpu.VMEM(x.shape, f32) for x in (mu, md) * 5),
            *(pltpu.VMEM(x.shape, f32) for x in (pn, pb, mn, mb, en, eb)),
            pltpu.VMEM((4, pn.shape[1]), f32),
            pltpu.VMEM((4, pn.shape[1]), f32),
            pltpu.VMEM((rows, lanes), f32),
            pltpu.VMEM((8, cols), f32),
            pltpu.VMEM((n, 2, rows), f32),
            pltpu.VMEM((n, 2, cols), f32),
            pltpu.SemaphoreType.DMA((12,)),
            pltpu.SemaphoreType.DMA((2, chunks)),
            pltpu.SemaphoreType.DMA((2, chunks)),
            pltpu.SemaphoreType.DMA((2, chunks)),
            pltpu.SemaphoreType.DMA((2,)),
            pltpu.SemaphoreType.DMA((2, n - 1)),
            pltpu.SemaphoreType.DMA((2, n - 1)),
            pltpu.SemaphoreType.DMA((2, pieces)),
            pltpu.SemaphoreType.DMA((2, pieces)),
        ],
        compiler_params=pltpu.CompilerParams(
            collective_id=0, has_side_effects=True, vmem_limit_bytes=40 * 2**20
        ),
        name="exchange",
    )(*held((pu[0], pd[0], *args[2:])))
    return tuple(pl.pallas_call(
        place_results,
        out_shape=[jax.ShapeDtypeStruct(shape, dtype) for shape, dtype in outs],
        in_specs=[vmem] * len(outs),
        out_specs=[hbm] * len(outs),
        scratch_shapes=[pltpu.SemaphoreType.DMA((len(outs),))],
        compiler_params=pltpu.CompilerParams(vmem_limit_bytes=2**20),
        name="place_results",
    )(*results))


def solution(mesh):
    in_specs = (
        P(("job", "dp"), None, "tp"),
        P(("job", "dp"), "tp", None),
        P(("job", "dp"), None),
        P(("job", "dp"), None),
        P(("job", "dp"), "tp"),
        P(("job", "tp"), "dp"),
        P(("job", "dp")),
        P(("job", "dp")),
        P(("job", "dp"), "tp"),
        P(("job", "tp"), "dp"),
        P(("job", "dp")),
        P(("job", "dp")),
    )
    out_specs = (
        P("job", "tp"),
        P(("job", "tp"), None),
        P("job"),
        P("job"),
        P(("job", "dp"), "tp"),
        P(("job", "tp"), "dp"),
        P(("job", "dp")),
        P(("job", "dp")),
        P(("job", "dp"), "tp"),
        P(("job", "tp"), "dp"),
        P(("job", "dp")),
        P(("job", "dp")),
    )
    return jax.shard_map(
        on_device if mesh.shape["dp"] != 2 else on_pair, mesh=mesh, in_specs=in_specs, out_specs=out_specs, check_vma=False
    )
```

```python
import functools

import jax
import jax.numpy as jnp
from jax import lax
from jax.experimental import pallas as pl
from jax.experimental.pallas import tpu as pltpu
from jax.sharding import PartitionSpec as P

learn_rate = 0.4
hold_rate = 0.9


def on_device(
    partial_up,
    partial_down,
    partial_norm,
    partial_bias,
    master_up,
    master_down,
    master_norm,
    master_bias,
    memory_up,
    memory_down,
    memory_norm,
    memory_bias,
):
    mean_up, mean_down = (
        lax.psum_scatter(partial_up[0], "dp", scatter_dimension=0, tiled=True),
        lax.psum_scatter(partial_down[0], "dp", scatter_dimension=1, tiled=True),
    )
    whole_norm, whole_bias = lax.psum((partial_norm[0], partial_bias[0]), "dp")
    place = lax.axis_index("dp")
    mean_norm = lax.dynamic_slice_in_dim(
        whole_norm, place * master_norm.shape[0], master_norm.shape[0]
    )
    mean_bias = lax.dynamic_slice_in_dim(
        whole_bias, place * master_bias.shape[0], master_bias.shape[0]
    )
    mean_rate = lax.axis_size("dp") ** (-0.5)
    mean_up = mean_up * mean_rate
    mean_down = mean_down * mean_rate
    mean_norm = mean_norm * mean_rate
    mean_bias = mean_bias * mean_rate
    own_up, own_down, slope_up_norm, slope_down_norm = lax.psum(
        (
            jnp.sum(master_up * master_up, axis=1, keepdims=True),
            jnp.sum(master_down * master_down, axis=0, keepdims=True),
            jnp.sum(mean_up * mean_up, axis=1, keepdims=True),
            jnp.sum(mean_down * mean_down, axis=0, keepdims=True),
        ),
        "tp",
    )
    mean_up = mean_up * (jnp.sqrt(own_up) * lax.rsqrt(slope_up_norm + 1e-06))
    mean_down = mean_down * (jnp.sqrt(own_down) * lax.rsqrt(slope_down_norm + 1e-06))
    state_new_up = hold_rate * memory_up + mean_up
    stepped_up = master_up - learn_rate * state_new_up
    state_new_down = hold_rate * memory_down + mean_down
    stepped_down = master_down - learn_rate * state_new_down
    state_new_norm = hold_rate * memory_norm + mean_norm
    stepped_norm = master_norm - learn_rate * state_new_norm
    state_new_bias = hold_rate * memory_bias + mean_bias
    stepped_bias = master_bias - learn_rate * state_new_bias
    compute_up, compute_down, compute_norm, compute_bias = (
        lax.all_gather(stepped_up.astype(jnp.bfloat16), "dp", axis=0, tiled=True),
        lax.all_gather(stepped_down.astype(jnp.bfloat16), "dp", axis=1, tiled=True),
        lax.all_gather(stepped_norm.astype(jnp.bfloat16), "dp", axis=0, tiled=True),
        lax.all_gather(stepped_bias.astype(jnp.bfloat16), "dp", axis=0, tiled=True),
    )
    return (
        compute_up,
        compute_down,
        compute_norm,
        compute_bias,
        stepped_up,
        stepped_down,
        stepped_norm,
        stepped_bias,
        state_new_up,
        state_new_down,
        state_new_norm,
        state_new_bias,
    )


chunks = 4
pieces = 4
lanes = 128


def lane_sums(x):
    total = x[:, :lanes]
    for at in range(lanes, x.shape[1], lanes):
        total = total + x[:, at : at + lanes]
    return total


def exchange(
    pu, pd, pn, pb, mu_h, md_h, mn, mb, eu_h, ed_h, en, eb,
    cu, cd, cn, cb, su, sd, sn, sb, tu, td, tn, tb,
    own_u, own_d, give_u, give_d, got_u, got_d, mu, md, eu, ed, pn_v, pb_v, mn_v, mb_v, en_v, eb_v, vec, got_vec,
    sq_u, acc_d, stat_u, stat_d,
    load_sem, give_sem, part_send, part_recv, vec_sem, stat_send, stat_recv, out_send, out_recv,
):
    me = lax.axis_index("dp")
    peer = 1 - me
    here = lax.axis_index("tp")
    n = lax.axis_size("tp")
    rate = lax.axis_size("dp") ** (-0.5)
    rows, wide = mu.shape
    tall, cols = md.shape
    part_u, part_d = rows // chunks, tall // chunks

    def mine(size):
        return pl.ds(pl.multiple_of(me * size, size), size)

    def theirs(size):
        return pl.ds(pl.multiple_of(peer * size, size), size)

    barrier = pltpu.get_barrier_semaphore()
    pl.semaphore_signal(barrier, inc=1, device_id={"dp": peer})
    for step in range(1, n):
        pl.semaphore_signal(barrier, inc=1, device_id={"tp": lax.rem(here + step, n)})

    give = []
    for at in range(chunks):
        span = pl.ds(at * part_u, part_u)
        give.append(pltpu.make_async_copy(
            pu.at[pl.ds(pl.multiple_of(peer * rows + at * part_u, 8), part_u), :],
            give_u.at[span, :],
            give_sem.at[0, at],
        ))
    for at in range(chunks):
        span = pl.ds(at * part_d, part_d)
        give.append(pltpu.make_async_copy(
            pd.at[span, theirs(cols)], give_d.at[span, :], give_sem.at[1, at]
        ))
    loads = [
        pltpu.make_async_copy(source, target, load_sem.at[at])
        for at, (source, target) in enumerate((
            (mu_h, mu),
            (md_h, md),
            (pu.at[mine(rows), :], own_u),
            (pd.at[:, mine(cols)], own_d),
            (eu_h, eu),
            (ed_h, ed),
            (pn, pn_v),
            (pb, pb_v),
            (mn, mn_v),
            (mb, mb_v),
            (en, en_v),
            (eb, eb_v),
        ))
    ]

    pl.semaphore_wait(barrier, n)

    send_u, send_d = [], []
    for at in range(chunks):
        span = pl.ds(at * part_u, part_u)
        send_u.append(pltpu.make_async_remote_copy(
            src_ref=pu.at[pl.ds(pl.multiple_of(peer * rows + at * part_u, 8), part_u), :],
            dst_ref=got_u.at[span, :],
            send_sem=part_send.at[0, at],
            recv_sem=part_recv.at[0, at],
            device_id={"dp": peer},
        ))
        span = pl.ds(at * part_d, part_d)
        send_d.append(pltpu.make_async_remote_copy(
            src_ref=pd.at[span, theirs(cols)],
            dst_ref=got_d.at[span, :],
            send_sem=part_send.at[1, at],
            recv_sem=part_recv.at[1, at],
            device_id={"dp": peer},
        ))
    for load, copy in zip(give[:chunks], send_u):
        copy.start()
    for load in (loads[0], loads[2], *loads[6:]):
        load.start()
    for load, copy in zip(give[chunks:], send_d):
        copy.start()
    for load in (loads[1], loads[3]):
        load.start()

    half = mn.shape[-1]
    for load in loads[6:]:
        load.wait()
    vec[0:1, :] = pn_v[...]
    vec[1:2, :] = pb_v[...]
    vec[2:3, :half] = mn_v[...].reshape(1, half)
    vec[2:3, half:] = en_v[...].reshape(1, half)
    vec[3:4, :half] = mb_v[...].reshape(1, half)
    vec[3:4, half:] = eb_v[...].reshape(1, half)

    step_u, step_d = 32, 64

    loads[0].wait()

    @pl.loop(0, rows // step_u)
    def _(at):
        span = pl.ds(pl.multiple_of(at * step_u, step_u), step_u)
        x = mu[span, :]
        sq_u[span, :] = lane_sums(x * x)

    stat_u[pl.ds(here, 1), 0:1, :] = jnp.sum(sq_u[...].T, axis=0).reshape(1, 1, rows)

    def down_squares(read, start, count):
        @pl.loop(0, count // step_d)
        def _(at):
            span = pl.ds(pl.multiple_of(start + at * step_d, step_d), step_d)
            x = read(span)
            acc_d[...] += jnp.sum((x * x).reshape(step_d // 8, 8, cols), axis=0)

    send_vec = pltpu.make_async_remote_copy(
        src_ref=vec, dst_ref=got_vec, send_sem=vec_sem.at[0], recv_sem=vec_sem.at[1],
        device_id={"dp": peer},
    )
    send_vec.start()

    loads[1].wait()
    acc_d[...] = jnp.zeros_like(acc_d)
    down_squares(lambda span: md[span, :], 0, tall)
    stat_d[pl.ds(here, 1), 0:1, :] = jnp.sum(acc_d[...], axis=0).reshape(1, 1, cols)
    acc_d[...] = jnp.zeros_like(acc_d)

    def to_peers(stat, which):
        copies = []
        for step in range(1, n):
            copies.append(pltpu.make_async_remote_copy(
                src_ref=stat.at[here],
                dst_ref=stat.at[here],
                send_sem=stat_send.at[which, step - 1],
                recv_sem=stat_recv.at[which, step - 1],
                device_id={"tp": lax.rem(here + step, n)},
            ))
        for copy in copies:
            copy.start()
        return copies

    loads[2].wait()
    for chunk in range(chunks):
        send_u[chunk].wait_recv()

        @pl.loop(0, part_u // step_u)
        def _(at):
            span = pl.ds(pl.multiple_of(chunk * part_u + at * step_u, step_u), step_u)
            x = (own_u[span, :] + got_u[span, :]) * rate
            own_u[span, :] = x
            sq_u[span, :] = lane_sums(x * x)

    stat_u[pl.ds(here, 1), 1:2, :] = jnp.sum(sq_u[...].T, axis=0).reshape(1, 1, rows)
    stats_u = to_peers(stat_u, 0)
    for load in loads[4:6]:
        load.start()

    loads[3].wait()

    def summed(span):
        x = (own_d[span, :] + got_d[span, :]) * rate
        own_d[span, :] = x
        return x

    for chunk in range(chunks):
        send_d[chunk].wait_recv()
        down_squares(summed, chunk * part_d, part_d)
    stat_d[pl.ds(here, 1), 1:2, :] = jnp.sum(acc_d[...], axis=0).reshape(1, 1, cols)
    stats_d = to_peers(stat_d, 1)

    send_vec.wait()
    mean = (vec[0:2, :] + got_vec[0:2, :]) * rate
    for at, (state, stepped, rounded) in enumerate(((tn, sn, cn), (tb, sb, cb))):
        row = slice(2 + at, 3 + at)
        low, high = mean[at : at + 1, :half], mean[at : at + 1, half:]
        new_own = hold_rate * vec[row, half:] + jnp.where(me == 0, low, high)
        own = vec[row, :half] - learn_rate * new_own
        new_other = hold_rate * got_vec[row, half:] + jnp.where(me == 0, high, low)
        other = got_vec[row, :half] - learn_rate * new_other
        state[...] = new_own.reshape(state.shape)
        stepped[...] = own.reshape(stepped.shape)
        whole = jnp.concatenate(
            [jnp.where(me == 0, own, other), jnp.where(me == 0, other, own)], axis=1
        )
        rounded[...] = whole.reshape(rounded.shape).astype(rounded.dtype)

    def ratio_of(stat):
        total = stat[0]
        for at in range(1, n):
            total = total + stat[at]
        return jnp.sqrt(total[0:1, :]) * lax.rsqrt(total[1:2, :] + 1e-06)

    loads[4].wait()
    for copy in stats_u:
        copy.wait()
    sq_u[...] = jnp.broadcast_to(ratio_of(stat_u), (lanes, rows)).T

    out = []
    for piece in range(pieces):
        size = rows // pieces

        @pl.loop(0, size // step_u)
        def _(at):
            start = piece * size + at * step_u
            span = pl.ds(pl.multiple_of(start, step_u), step_u)
            ratio = sq_u[span, :]
            ratio = jnp.concatenate([ratio] * (wide // lanes), axis=1)
            state = hold_rate * eu[span, :] + own_u[span, :] * ratio
            stepped = mu[span, :] - learn_rate * state
            tu[span, :] = state
            su[span, :] = stepped
            place = pl.ds(pl.multiple_of(me * rows + start, step_u), step_u)
            cu[place, :] = stepped.astype(cu.dtype)

        span = pl.ds(pl.multiple_of(me * rows + piece * size, step_u), size)
        out.append(pltpu.make_async_remote_copy(
            src_ref=cu.at[span, :],
            dst_ref=cu.at[span, :],
            send_sem=out_send.at[0, piece],
            recv_sem=out_recv.at[0, piece],
            device_id={"dp": peer},
        ))
        out[-1].start()

    loads[5].wait()
    for copy in stats_d:
        copy.wait()
    ratio_d = ratio_of(stat_d)
    acc_d[...] = jnp.broadcast_to(ratio_d, acc_d.shape)
    for piece in range(pieces):
        size = tall // pieces

        @pl.loop(0, size // step_d)
        def _(at):
            span = pl.ds(pl.multiple_of(piece * size + at * step_d, step_d), step_d)
            ratio = jnp.broadcast_to(acc_d[...][None], (step_d // 8, 8, cols)).reshape(step_d, cols)
            state = hold_rate * ed[span, :] + own_d[span, :] * ratio
            stepped = md[span, :] - learn_rate * state
            td[span, :] = state
            sd[span, :] = stepped
            cd[span, mine(cols)] = stepped.astype(cd.dtype)

        span = pl.ds(piece * size, size)
        out.append(pltpu.make_async_remote_copy(
            src_ref=cd.at[span, mine(cols)],
            dst_ref=cd.at[span, mine(cols)],
            send_sem=out_send.at[1, piece],
            recv_sem=out_recv.at[1, piece],
            device_id={"dp": peer},
        ))
        out[-1].start()

    for copy in send_u + send_d:
        copy.wait_send()
    for copy in out:
        copy.wait()


def place_results(*refs):
    count = (len(refs) - 1) // 2
    sem = refs[-1]
    copies = [
        pltpu.make_async_copy(refs[at], refs[count + at], sem.at[at]) for at in range(count)
    ]
    for copy in copies:
        copy.start()
    for copy in copies:
        copy.wait()


def held(arrays):
    return [pltpu.with_memory_space_constraint(x, pltpu.HBM) for x in arrays]


def on_pair(*args):
    pu, pd, pn, pb, mu, md, mn, mb, eu, ed, en, eb = args
    n = lax.axis_size("tp")
    f32, bf16 = jnp.float32, jnp.bfloat16
    vmem = pl.BlockSpec(memory_space=pltpu.VMEM)
    hbm = pl.BlockSpec(memory_space=pltpu.HBM)
    wide, tall = pu.shape[2], pd.shape[1]
    outs = (
        ((pu.shape[1], wide), bf16),
        ((tall, pd.shape[2]), bf16),
        ((pn.shape[1],), bf16),
        ((pb.shape[1],), bf16),
        *((x.shape, f32) for x in (mu, md, mn, mb)),
        *((x.shape, f32) for x in (mu, md, mn, mb)),
    )
    rows, cols = mu.shape[0], md.shape[1]
    results = pl.pallas_call(
        exchange,
        out_shape=[jax.ShapeDtypeStruct(shape, dtype) for shape, dtype in outs],
        in_specs=[hbm] * len(args),
        out_specs=[vmem] * len(outs),
        scratch_shapes=[
            *(pltpu.VMEM(x.shape, f32) for x in (mu, md) * 5),
            *(pltpu.VMEM(x.shape, f32) for x in (pn, pb, mn, mb, en, eb)),
            pltpu.VMEM((4, pn.shape[1]), f32),
            pltpu.VMEM((4, pn.shape[1]), f32),
            pltpu.VMEM((rows, lanes), f32),
            pltpu.VMEM((8, cols), f32),
            pltpu.VMEM((n, 2, rows), f32),
            pltpu.VMEM((n, 2, cols), f32),
            pltpu.SemaphoreType.DMA((12,)),
            pltpu.SemaphoreType.DMA((2, chunks)),
            pltpu.SemaphoreType.DMA((2, chunks)),
            pltpu.SemaphoreType.DMA((2, chunks)),
            pltpu.SemaphoreType.DMA((2,)),
            pltpu.SemaphoreType.DMA((2, n - 1)),
            pltpu.SemaphoreType.DMA((2, n - 1)),
            pltpu.SemaphoreType.DMA((2, pieces)),
            pltpu.SemaphoreType.DMA((2, pieces)),
        ],
        compiler_params=pltpu.CompilerParams(
            collective_id=0, has_side_effects=True, vmem_limit_bytes=40 * 2**20
        ),
        name="exchange",
    )(*held((pu[0], pd[0], *args[2:])))
    return tuple(pl.pallas_call(
        place_results,
        out_shape=[jax.ShapeDtypeStruct(shape, dtype) for shape, dtype in outs],
        in_specs=[vmem] * len(outs),
        out_specs=[hbm] * len(outs),
        scratch_shapes=[pltpu.SemaphoreType.DMA((len(outs),))],
        compiler_params=pltpu.CompilerParams(vmem_limit_bytes=2**20),
        name="place_results",
    )(*results))


def solution(mesh):
    in_specs = (
        P(("job", "dp"), None, "tp"),
        P(("job", "dp"), "tp", None),
        P(("job", "dp"), None),
        P(("job", "dp"), None),
        P(("job", "dp"), "tp"),
        P(("job", "tp"), "dp"),
        P(("job", "dp")),
        P(("job", "dp")),
        P(("job", "dp"), "tp"),
        P(("job", "tp"), "dp"),
        P(("job", "dp")),
        P(("job", "dp")),
    )
    out_specs = (
        P("job", "tp"),
        P(("job", "tp"), None),
        P("job"),
        P("job"),
        P(("job", "dp"), "tp"),
        P(("job", "tp"), "dp"),
        P(("job", "dp")),
        P(("job", "dp")),
        P(("job", "dp"), "tp"),
        P(("job", "tp"), "dp"),
        P(("job", "dp")),
        P(("job", "dp")),
    )
    return jax.shard_map(
        on_device if mesh.shape["dp"] != 2 else on_pair, mesh=mesh, in_specs=in_specs, out_specs=out_specs, check_vma=False
    )
```
